32 devices in a mesh: pts: 8 (over y, x, core), wid: 4 (over z).
Axes of the slice: x: 2, y: 2, z: 4, core: 2. Of those that a mesh axis runs over, the one named last changes fastest.
Arguments:
- vertex_features: bfloat16 [90112, 512], P('pts'), may hold values from -40 to 40, as said below
- entry_matrix: bfloat16 [512, 512], P(None, 'wid'), may hold values from -2 to 2, as said below
- partition_matrix: bfloat16 [64, 32], replicated, may hold values from -3 to 3, as said below
- sharpness_matrix: float32 [64], replicated, may hold values from -3 to 3, as said below
- summary_qkv_matrix: float32 [3, 64, 64], replicated, may hold values from -3 to 3
- exit_matrix: bfloat16 [512, 512], P('wid'), may hold values from -0.5 to 0.5
- widening_matrix: bfloat16 [512, 512], P('wid'), may hold values from -0.25 to 0.25
- narrowing_matrix: bfloat16 [512, 512], P('wid'), may hold values from -0.25 to 0.25
Outputs:
- result: bfloat16 [90112, 512], P(('pts', 'wid'))
The draws below stay inside these ranges and needn't reach their ends.
Inputs may be any that keep to these rules, and one draw needn't show every extreme that they name: `vertex_features`: features of the points, of order one to ten. `entry_matrix`: weights of the point projection. `partition_matrix`: slice logit weights. `sharpness_matrix`: temperature weights.
All inputs are finite; a program needn't handle non-finite values.
Results may differ from the reference program's by a relative error of at most 0.013.
Values may be sent and summed in bfloat16 or wider, within the bound.
A program may use at most 128 MiB of HBM per device.

```python
import jax
import jax.numpy as jnp
from jax import lax

D = 512
H = 8
DH = 64
G = 32
FF = 512
NPOINTS = 90112


def draw_vertex_features(key, part):
    key_base = jax.random.fold_in(key, 11)
    key_dir = jax.random.fold_in(key, 12)
    key_scale = jax.random.fold_in(key, 13)
    base = jnp.clip(jax.random.normal(key_base, (NPOINTS, D), jnp.float32), -4.0, 4.0)
    spread = jnp.exp(jax.random.uniform(key_scale, (NPOINTS, 1), jnp.float32, 0.0, 1.1))
    direction = jnp.clip(jax.random.normal(key_dir, (1, D), jnp.float32), -4.0, 4.0)
    ramp = 1.0 + 2.0 * jnp.arange(NPOINTS, dtype=jnp.float32)[:, None] / jnp.float32(max(NPOINTS - 1, 1))
    values = base * jnp.minimum(spread, 3.0) + ramp * direction
    values = 0.5 * values
    return jnp.clip(values, -40.0, 40.0).astype(jnp.bfloat16)


def draw_entry_matrix(key, part):
    noise = jnp.clip(jax.random.normal(jax.random.fold_in(key, 21), (D, D), jnp.float32), -6.0, 6.0) / jnp.sqrt(jnp.float32(D))
    return jnp.clip(noise, -2.0, 2.0).astype(jnp.bfloat16)


def draw_partition_matrix(key, part):
    rough = jax.random.normal(jax.random.fold_in(key, 31), (DH, G), jnp.float32)
    values = 0.8 * rough
    return jnp.clip(values, -3.0, 3.0).astype(jnp.bfloat16)


def draw_sharpness_matrix(key, part):
    rough = jax.random.normal(jax.random.fold_in(key, 41), (DH,), jnp.float32)
    values = 0.6 * rough
    return jnp.clip(values, -3.0, 3.0).astype(jnp.float32)


def draw_summary_qkv_matrix(key, part):
    rough = jax.random.normal(jax.random.fold_in(key, 51), (3, DH, DH), jnp.float32)
    values = 0.55 * rough
    return jnp.clip(values, -3.0, 3.0).astype(jnp.float32)


def block_scale(rng, shape, shards, least, top_value):
    level = 1.0
    for axis_at, parts in shards:
        steps = jax.random.uniform(jax.random.fold_in(jax.random.fold_in(rng, 6), axis_at), (parts,), jnp.float32, least / len(shards), top_value / len(shards))
        level = level * jnp.repeat(jnp.exp(steps), shape[axis_at] // parts).reshape((-1,) + (1,) * (len(shape) - 1 - axis_at))
    return level


def normal_values(stream_key, extent, deviation, most, pieces=(), held_as=jnp.bfloat16):
    result = jax.random.normal(stream_key, extent, jnp.float32) * deviation
    if len(pieces) > 0:
        result = block_scale(stream_key, extent, pieces, -0.22, 0.18) * result
    return jnp.clip(result, min=-most, max=most).astype(held_as)


def setup_inputs(seed: int = 0) -> dict:
    arg_keys = jax.random.split(jax.random.key(seed), 9)
    return {
        "vertex_features": draw_vertex_features(jax.random.fold_in(arg_keys[8], 71), 0),
        "entry_matrix": draw_entry_matrix(jax.random.fold_in(arg_keys[8], 71), 0),
        "partition_matrix": draw_partition_matrix(jax.random.fold_in(arg_keys[8], 71), 0),
        "sharpness_matrix": draw_sharpness_matrix(jax.random.fold_in(arg_keys[8], 71), 0),
        "summary_qkv_matrix": draw_summary_qkv_matrix(jax.random.fold_in(arg_keys[8], 71), 0),
        "exit_matrix": normal_values(arg_keys[5], (D, D), (D // 4) ** -0.5, 0.5, ((0, 4),)),
        "widening_matrix": normal_values(arg_keys[6], (D, FF), D ** -0.5, 0.25, ((0, 4),)),
        "narrowing_matrix": normal_values(arg_keys[7], (FF, D), FF ** -0.5, 0.25, ((0, 4),)),
    }


def layer_norm(values):
    centred = values - lax.optimization_barrier(jnp.mean(values, axis=-1, keepdims=True))
    variance = lax.optimization_barrier(jnp.mean(centred * centred, axis=-1, keepdims=True))
    return centred * lax.rsqrt(variance + 1e-05)

def reference(vertex_features, entry_matrix, partition_matrix, sharpness_matrix, summary_qkv_matrix, exit_matrix, widening_matrix, narrowing_matrix):
    features = vertex_features.astype(jnp.float32)
    normed = layer_norm(features).astype(jnp.bfloat16)
    feats = jnp.dot(normed, entry_matrix, preferred_element_type=jnp.float32).astype(jnp.bfloat16)
    attention_cluster = feats.reshape(feats.shape[0], H, DH).astype(jnp.float32)
    partition_sharpness = 0.5 + jax.nn.softplus(jnp.einsum('kgv,v->kg', attention_cluster, sharpness_matrix))
    partition_scores = jnp.einsum('nhd,dg->nhg', attention_cluster, partition_matrix.astype(jnp.float32))
    partition_mapping = jax.nn.softmax(partition_scores / partition_sharpness[:, :, None], axis=-1).astype(jnp.bfloat16)
    weights32 = partition_mapping.astype(jnp.float32)
    numerator = jnp.einsum('nhg,nhd->hgd', weights32, attention_cluster)
    mass = lax.optimization_barrier(jnp.sum(weights32, axis=0))
    token_rows = numerator / (mass[:, :, None] + 1e-05)
    hp = lax.Precision.HIGHEST
    queries = jnp.einsum('hgd,de->hge', token_rows, summary_qkv_matrix[0], precision=hp)
    keys_all = jnp.einsum('hgd,de->hge', token_rows, summary_qkv_matrix[1], precision=hp)
    value_rows_total = jnp.einsum('hgd,de->hge', token_rows, summary_qkv_matrix[2], precision=hp)
    scores = jnp.einsum('hge,hke->hgk', queries, keys_all, precision=hp) / jnp.sqrt(jnp.float32(DH))
    attend = jax.nn.softmax(scores, axis=-1)
    out_tok = jnp.einsum('hgk,hke->hge', attend, value_rows_total, precision=hp).astype(jnp.bfloat16)
    deslice = jnp.einsum('nhg,hgd->nhd', weights32, out_tok.astype(jnp.float32)).astype(jnp.bfloat16)
    deslice = deslice.reshape(feats.shape[0], D)
    midway = features + jnp.dot(deslice, exit_matrix, preferred_element_type=jnp.float32)
    normed2 = layer_norm(midway).astype(jnp.bfloat16)
    hidden = jax.nn.gelu(jnp.dot(normed2, widening_matrix, preferred_element_type=jnp.float32)).astype(jnp.bfloat16)
    return (midway + jnp.dot(hidden, narrowing_matrix, preferred_element_type=jnp.float32)).astype(jnp.bfloat16)
```

```python
import functools

import jax
import jax.numpy as jnp
from jax import lax
from jax.experimental import pallas as pl
from jax.experimental.pallas import tpu as pltpu
from jax.sharding import PartitionSpec as P

MESH = pl.DeviceIdType.MESH
F32 = jnp.float32
BF16 = jnp.bfloat16
SHARE = 2


def layer_norm(values):
    centred = values - jnp.mean(values, axis=-1, keepdims=True)
    variance = jnp.mean(centred * centred, axis=-1, keepdims=True)
    return centred * lax.rsqrt(variance + 1e-05)


def pick_tile(rows, choices):
    for choice in choices:
        if rows % choice == 0:
            return choice
    return rows


def gather_kernel(
    sizes, x_ref, ent_ref, part_ref, sharp_ref, ex_ref, up_ref, dn_ref,
    w_ref, red_ref, exg_ref, upg_ref, dng_ref,
    rows_buf, ent_buf, entt_buf, logit_mat, num_buf, mass_buf,
    piece_all, piece_in, piece_sum, ring_in, fin_buf,
    x_sem, own_sem, zs_sem, zr_sem, fs_sem, fr_sem,
    rs_send, rs_recv, z_send, z_recv, ag_send, ag_recv,
):
    pts, wid, share, tile, head, slices, heads = sizes
    p, w = lax.axis_index("pts"), lax.axis_index("wid")
    rows = rows_buf.shape[0]
    tiles = rows // tile
    group, member = p // share, p % share

    x_copy = pltpu.make_async_copy(
        x_ref.at[pl.ds(pl.multiple_of(w * rows, rows), rows)], rows_buf, x_sem
    )
    x_copy.start()

    barrier = pltpu.get_barrier_semaphore()
    for d in range(1, wid):
        pl.semaphore_signal(
            barrier, inc=1, device_id=(p, lax.rem(w + d, wid)), device_id_type=MESH
        )
    for d in range(1, pts):
        pl.semaphore_signal(
            barrier, inc=1, device_id=(lax.rem(p + d, pts), w), device_id_type=MESH
        )
    pl.semaphore_wait(barrier, wid - 1 + pts - 1)

    chunk = ex_ref.shape[0]
    ent_part = ent_ref.shape[0] // share
    out_part = chunk // share

    def spot(m, owner, part):
        if m == 0:
            return ent_buf.at[owner, pl.ds(pl.multiple_of(part * ent_part, ent_part), ent_part)]
        full = (exg_ref, upg_ref, dng_ref)[m - 1]
        return full.at[pl.ds(pl.multiple_of(owner * chunk + part * out_part, out_part), out_part)]

    def mine(m):
        if m == 0:
            return ent_ref.at[pl.ds(pl.multiple_of(member * ent_part, ent_part), ent_part)]
        own = (ex_ref, up_ref, dn_ref)[m - 1]
        return own.at[pl.ds(pl.multiple_of(member * out_part, out_part), out_part)]

    def across(m, d):
        return pltpu.make_async_remote_copy(
            src_ref=mine(m), dst_ref=spot(m, w, member),
            send_sem=zs_sem.at[m, d - 1], recv_sem=zr_sem.at[m, d - 1],
            device_id=(p, lax.rem(w + d, wid)), device_id_type=MESH,
        )

    def forward(m, d, e):
        owner = lax.rem(w - d + wid, wid)
        return pltpu.make_async_remote_copy(
            src_ref=spot(m, owner, member), dst_ref=spot(m, owner, member),
            send_sem=fs_sem.at[m, d - 1, e - 1], recv_sem=fr_sem.at[m, d - 1, e - 1],
            device_id=(group * share + lax.rem(member + e, share), w), device_id_type=MESH,
        )

    crossing = [[across(m, d) for d in range(1, wid)] for m in range(4)]
    for m in range(4):
        for copy in crossing[m]:
            copy.start()
    own_copies = []
    for m in range(1, 4):
        full = (exg_ref, upg_ref, dng_ref)[m - 1]
        copy = pltpu.make_async_copy(
            (ex_ref, up_ref, dn_ref)[m - 1],
            full.at[pl.ds(pl.multiple_of(w * chunk, chunk), chunk)], own_sem.at[m - 1],
        )
        copy.start()
        own_copies.append(copy)

    held = logit_mat.shape[1] // head
    wide = held * slices
    logit_mat[...] = jnp.zeros_like(logit_mat)
    part_t = part_ref[...].astype(F32).T
    sharp = sharp_ref[...]
    sharp_hi = sharp.astype(BF16).astype(F32)
    sharp_lo = sharp - sharp_hi
    for h in range(held):
        lanes = slice(h * head, (h + 1) * head)
        logit_mat[h * slices:(h + 1) * slices, lanes] = part_t
        logit_mat[wide + h:wide + h + 1, lanes] = sharp_hi
        logit_mat[wide + 8 + h:wide + 8 + h + 1, lanes] = sharp_lo
    num_buf[...] = jnp.zeros_like(num_buf)
    mass_buf[...] = jnp.zeros_like(mass_buf)
    x_copy.wait()

    def norm_step(t, carry):
        at = pl.ds(pl.multiple_of(t * tile, tile), tile)
        rows_buf[at, :] = layer_norm(rows_buf[at, :].astype(F32)).astype(BF16)
        return carry

    lax.fori_loop(0, tiles, norm_step, 0)

    def pass_on(m):
        copies = []
        for d in range(1, wid):
            crossing[m][d - 1].wait_recv()
            for e in range(1, share):
                copy = forward(m, d, e)
                copy.start()
                copies.append(copy)
        return copies

    width = ent_ref.shape[1]
    passed = [pass_on(0)]
    for copy in passed[0]:
        copy.wait_recv()
    own_at = pl.ds(pl.multiple_of(w * width, width), width)
    entt_buf[own_at, :] = ent_ref[...].T
    for d in range(1, wid):
        owner = lax.rem(w - d + wid, wid)
        entt_buf[pl.ds(pl.multiple_of(owner * width, width), width), :] = ent_buf[owner].T

    lhs = logit_mat[...].astype(BF16)
    groups = heads // held
    both = (((1,), (1,)), ((), ()))

    def slice_step(t, carry):
        at = pl.ds(pl.multiple_of(t * tile, tile), tile)
        feats = lax.dot_general(
            entt_buf[...], rows_buf[at, :], both, preferred_element_type=F32
        ).astype(BF16)
        for gi in range(groups):
            own = feats[gi * held * head:(gi + 1) * held * head]
            logits = jnp.dot(lhs, own, preferred_element_type=F32)
            raw = logits[wide:wide + 8] + logits[wide + 8:wide + 16]
            soft = jnp.maximum(raw, 0.0) + jnp.log1p(jnp.exp(-jnp.abs(raw)))
            inverse = 1.0 / (0.5 + soft)
            weights = []
            for h in range(held):
                score = logits[h * slices:(h + 1) * slices] * inverse[h:h + 1]
                power = jnp.exp(score - jnp.max(score, axis=0, keepdims=True))
                weights.append(power * (1.0 / jnp.sum(power, axis=0, keepdims=True)))
            block = jnp.concatenate(weights, axis=0).astype(BF16)
            num_buf[gi] += lax.dot_general(block, own, both, preferred_element_type=F32)
            rounded = block.astype(F32)
            mass = rounded[:, :128]
            for c in range(1, tile // 128):
                mass = mass + rounded[:, c * 128:(c + 1) * 128]
            mass_buf[gi * wide:(gi + 1) * wide] += mass
            w_ref[at, gi * wide:(gi + 1) * wide] = block.T
        return carry

    lax.fori_loop(0, tiles, slice_step, 0)

    lane = lax.broadcasted_iota(jnp.int32, (slices, 2 * head), 1)
    for h in range(heads):
        gi, k = h // held, h % held
        block = num_buf[gi, k * slices:(k + 1) * slices, (k // 2) * 2 * head:(k // 2 + 1) * 2 * head]
        if k % 2:
            block = pltpu.roll(block, head, 1)
        mass = jnp.sum(mass_buf[h * slices:(h + 1) * slices], axis=1, keepdims=True)
        piece_all[h * slices:(h + 1) * slices] = jnp.where(lane < head, block, mass)

    size = heads * slices // pts

    def piece(ref, owner):
        return ref.at[pl.ds(pl.multiple_of(owner * size, size), size)]

    scatter = []
    for d in range(1, pts):
        to = lax.rem(p + d, pts)
        scatter.append(pltpu.make_async_remote_copy(
            src_ref=piece(piece_all, to), dst_ref=piece_in.at[d - 1],
            send_sem=rs_send.at[d - 1], recv_sem=rs_recv.at[d - 1],
            device_id=(to, w), device_id_type=MESH,
        ))
    for copy in scatter:
        copy.start()
    passed += [pass_on(m) for m in range(1, 4)]
    total = piece_all[pl.ds(pl.multiple_of(p * size, size), size)]
    for d in range(1, pts):
        scatter[d - 1].wait_recv()
        total = total + piece_in[d - 1]
    piece_sum[...] = total
    ring = []
    for d in range(1, wid):
        ring.append(pltpu.make_async_remote_copy(
            src_ref=piece_sum, dst_ref=ring_in.at[d - 1],
            send_sem=z_send.at[d - 1], recv_sem=z_recv.at[d - 1],
            device_id=(p, lax.rem(w + d, wid)), device_id_type=MESH,
        ))
    for copy in ring:
        copy.start()
    for d in range(1, wid):
        ring[d - 1].wait_recv()
        total = total + ring_in[d - 1]
    fin_buf[pl.ds(pl.multiple_of(p * size, size), size)] = total
    spread = []
    for d in range(1, pts):
        spread.append(pltpu.make_async_remote_copy(
            src_ref=piece(fin_buf, p), dst_ref=piece(fin_buf, p),
            send_sem=ag_send.at[d - 1], recv_sem=ag_recv.at[d - 1],
            device_id=(lax.rem(p + d, pts), w), device_id_type=MESH,
        ))
    for copy in spread:
        copy.start()
    for copy in spread:
        copy.wait_recv()
    red_ref[...] = fin_buf[...]
    for m in range(1, 4):
        for copy in passed[m]:
            copy.wait_recv()
    for copy in own_copies:
        copy.wait()
    for copies in crossing + passed + [scatter, ring, spread]:
        for copy in copies:
            copy.wait_send()


def rows_kernel(
    sizes, at_ref, red_ref, qkv_ref, w_ref, x_ref, exg_ref, upg_ref, dng_ref, out_ref, mix_buf
):
    head, slices, heads = sizes

    @pl.when(pl.program_id(0) == 0)
    def _():
        high = lax.Precision.HIGHEST
        count = heads * slices
        red = red_ref[...]
        tokens = red[:, :head] / (red[:, head:] + 1e-05)
        queries, keys_all, value_rows = (
            jnp.dot(tokens, qkv_ref[i], precision=high, preferred_element_type=F32)
            for i in range(3)
        )
        scores = lax.dot_general(
            queries, keys_all, (((1,), (1,)), ((), ())), precision=high,
            preferred_element_type=F32,
        ) * (1.0 / head ** 0.5)
        row = lax.broadcasted_iota(jnp.int32, (count, count), 0) // slices
        col = lax.broadcasted_iota(jnp.int32, (count, count), 1) // slices
        scores = jnp.where(row == col, scores, -jnp.inf)
        power = jnp.exp(scores - jnp.max(scores, axis=1, keepdims=True))
        attend = power / jnp.sum(power, axis=1, keepdims=True)
        out_tok = jnp.dot(attend, value_rows, precision=high, preferred_element_type=F32)
        spread = jnp.concatenate([out_tok] * heads, axis=1)
        row = lax.broadcasted_iota(jnp.int32, spread.shape, 0) // slices
        col = lax.broadcasted_iota(jnp.int32, spread.shape, 1) // head
        spread = jnp.where(row == col, spread, 0.0).astype(BF16)
        mix_buf[...] = jnp.dot(
            spread, exg_ref[...], preferred_element_type=F32
        ).astype(BF16)

    midway = x_ref[...].astype(F32) + jnp.dot(
        w_ref[...], mix_buf[...], preferred_element_type=F32
    )
    normed = layer_norm(midway).astype(BF16)
    hidden = jax.nn.gelu(jnp.dot(normed, upg_ref[...], preferred_element_type=F32)).astype(BF16)
    out_ref[...] = (
        midway + jnp.dot(hidden, dng_ref[...], preferred_element_type=F32)
    ).astype(BF16)


def local(x, entry, partition, sharpness, qkv, exit_m, widening, narrowing):
    pts, wid = lax.axis_size("pts"), lax.axis_size("wid")
    width = x.shape[1]
    head, slices = partition.shape
    heads = entry.shape[1] * wid // head
    rows = x.shape[0] // wid
    chunk = exit_m.shape[0]
    cells = heads * slices
    tile = pick_tile(rows, (256, 128))
    held = 256 // head
    size = cells // pts
    share = SHARE
    sizes = (pts, wid, share, tile, head, slices, heads)
    vmem = pl.BlockSpec(memory_space=pltpu.VMEM)
    hbm = pl.BlockSpec(memory_space=pl.ANY)
    dma = pltpu.SemaphoreType.DMA
    full = jax.ShapeDtypeStruct((chunk * wid, width), BF16)
    weights, reduced, exg, upg, dng = pl.pallas_call(
        functools.partial(gather_kernel, sizes),
        name="slices_and_gather",
        out_shape=(
            jax.ShapeDtypeStruct((rows, cells), BF16),
            jax.ShapeDtypeStruct((cells, 2 * head), F32),
            full, full, full,
        ),
        in_specs=[hbm] + [vmem] * 6,
        out_specs=(vmem, vmem, hbm, hbm, hbm),
        scratch_shapes=[
            pltpu.VMEM((rows, width), BF16),
            pltpu.VMEM((wid,) + entry.shape, BF16),
            pltpu.VMEM((entry.shape[1] * wid, entry.shape[0]), BF16),
            pltpu.VMEM((held * slices + 16, held * head), F32),
            pltpu.VMEM((heads // held, held * slices, held * head), F32),
            pltpu.VMEM((cells, 128), F32),
            pltpu.VMEM((cells, 2 * head), F32),
            pltpu.VMEM((pts - 1, size, 2 * head), F32),
            pltpu.VMEM((size, 2 * head), F32),
            pltpu.VMEM((wid - 1, size, 2 * head), F32),
            pltpu.VMEM((cells, 2 * head), F32),
            dma, dma((3,)),
            dma((4, wid - 1)), dma((4, wid - 1)),
            dma((4, wid - 1, share - 1)), dma((4, wid - 1, share - 1)),
            dma((pts - 1,)), dma((pts - 1,)),
            dma((wid - 1,)), dma((wid - 1,)),
            dma((pts - 1,)), dma((pts - 1,)),
        ],
        compiler_params=pltpu.CompilerParams(
            collective_id=0, has_side_effects=True, vmem_limit_bytes=40 * 1024 * 1024
        ),
    )(x, entry, partition, sharpness.reshape(1, head), exit_m, widening, narrowing)

    step = pick_tile(rows, (704, 256, 128))
    steps = rows // step
    whole = lambda a: pl.BlockSpec(a.shape, lambda i, at: (0,) * a.ndim)
    at = lax.axis_index("wid").astype(jnp.int32).reshape(1)
    return pl.pallas_call(
        functools.partial(rows_kernel, (head, slices, heads)),
        name="mix_and_feed",
        out_shape=jax.ShapeDtypeStruct((rows, width), BF16),
        grid_spec=pltpu.PrefetchScalarGridSpec(
            num_scalar_prefetch=1,
            grid=(steps,),
            in_specs=[
                whole(reduced),
                whole(qkv),
                pl.BlockSpec((step, cells), lambda i, at: (i, 0)),
                pl.BlockSpec((step, width), lambda i, at: (at[0] * steps + i, 0)),
                whole(exg), whole(upg), whole(dng),
            ],
            out_specs=pl.BlockSpec((step, width), lambda i, at: (i, 0)),
            scratch_shapes=[pltpu.VMEM((cells, width), BF16)],
        ),
        compiler_params=pltpu.CompilerParams(
            dimension_semantics=("arbitrary",), vmem_limit_bytes=48 * 1024 * 1024
        ),
    )(at, reduced, qkv, weights, x, exg, upg, dng)


def solution(mesh):
    placed = (
        P("pts", None),
        P(None, "wid"),
        P(),
        P(),
        P(),
        P("wid", None),
        P("wid", None),
        P("wid", None),
    )
    return jax.shard_map(
        local, mesh=mesh, in_specs=placed, out_specs=P(("pts", "wid"), None), check_vma=False
    )
```

```python
import functools

import jax
import jax.numpy as jnp
from jax import lax
from jax.experimental import pallas as pl
from jax.experimental.pallas import tpu as pltpu
from jax.sharding import PartitionSpec as P

MESH = pl.DeviceIdType.MESH
F32 = jnp.float32
BF16 = jnp.bfloat16


def layer_norm(values):
    centred = values - jnp.mean(values, axis=-1, keepdims=True)
    variance = jnp.mean(centred * centred, axis=-1, keepdims=True)
    return centred * lax.rsqrt(variance + 1e-05)


def pick_tile(rows, choices):
    for choice in choices:
        if rows % choice == 0:
            return choice
    return rows


def gather_kernel(
    sizes, x_ref, ent_ref, part_hbm, sharp_hbm, ex_ref, up_ref, dn_ref,
    w_ref, red_ref, exg_ref, upg_ref, dng_ref,
    rows_buf, ent_buf, entt_buf, logit_mat, num_buf, mass_buf,
    piece_all, piece_in, piece_sum, ring_in, fin_buf, part_ref, sharp_ref,
    x_sem, own_sem, zs_sem, zr_sem, fs_sem, fr_sem, cs_sem, cr_sem,
    rs_send, rs_recv, z_send, z_recv, ag_send, ag_recv,
):
    pts, wid, share, tile, head, slices, heads = sizes
    p, w = lax.axis_index("pts"), lax.axis_index("wid")
    rows = rows_buf.shape[0]
    tiles = rows // tile
    norm_tile = pick_tile(rows, (704, 256, 128))
    norm_tiles = rows // norm_tile
    chips = share // 2
    group, core = p // share, p % 2
    chip = (p % share) // 2
    member = core * chips + chip

    x_copy = pltpu.make_async_copy(
        x_ref.at[pl.ds(pl.multiple_of(w * rows, rows), rows)], rows_buf, x_sem
    )
    x_copy.start()

    small_copies = [
        pltpu.make_async_copy(part_hbm, part_ref, own_sem.at[0]),
        pltpu.make_async_copy(sharp_hbm, sharp_ref, own_sem.at[1]),
        pltpu.make_async_copy(ent_ref, ent_buf.at[w], own_sem.at[2]),
    ]
    for copy in small_copies:
        copy.start()

    barrier = pltpu.get_barrier_semaphore()
    for d in range(1, wid):
        pl.semaphore_signal(
            barrier, inc=1, device_id=(p, lax.rem(w + d, wid)), device_id_type=MESH
        )
    for d in range(1, pts):
        pl.semaphore_signal(
            barrier, inc=1, device_id=(lax.rem(p + d, pts), w), device_id_type=MESH
        )
    pl.semaphore_wait(barrier, wid - 1 + pts - 1)

    chunk = ex_ref.shape[0]
    ent_part = ent_ref.shape[0] // share
    out_part = chunk // share

    def spot(m, owner, part, parts=1):
        if m == 0:
            count = ent_part * parts
            return ent_buf.at[owner, pl.ds(pl.multiple_of(part * count, count), count)]
        count = out_part * parts
        full = (exg_ref, upg_ref, dng_ref)[m - 1]
        return full.at[pl.ds(pl.multiple_of(owner * chunk + part * count, count), count)]

    def mine(m):
        if m == 0:
            return spot(0, w, member)
        own = (ex_ref, up_ref, dn_ref)[m - 1]
        return own.at[pl.ds(pl.multiple_of(member * out_part, out_part), out_part)]

    def across(m, d):
        return pltpu.make_async_remote_copy(
            src_ref=mine(m), dst_ref=spot(m, w, member),
            send_sem=zs_sem.at[m, d - 1], recv_sem=zr_sem.at[m, d - 1],
            device_id=(p, lax.rem(w + d, wid)), device_id_type=MESH,
        )

    def forward(m, d, e):
        owner = lax.rem(w - d + wid, wid)
        to = group * share + 2 * lax.rem(chip + e, chips) + core
        return pltpu.make_async_remote_copy(
            src_ref=spot(m, owner, member), dst_ref=spot(m, owner, member),
            send_sem=fs_sem.at[m, d - 1, e - 1], recv_sem=fr_sem.at[m, d - 1, e - 1],
            device_id=(to, w), device_id_type=MESH,
        )

    def swap(m, d):
        owner = lax.rem(w - d + wid, wid)
        half = spot(m, owner, core, chips)
        return pltpu.make_async_remote_copy(
            src_ref=half, dst_ref=half,
            send_sem=cs_sem.at[m, d - 1], recv_sem=cr_sem.at[m, d - 1],
            device_id=(p + 1 - 2 * core, w), device_id_type=MESH,
        )

    small_copies[2].wait()
    crossing = [[across(m, d) for d in range(1, wid)] for m in range(4)]
    for m in range(4):
        for copy in crossing[m]:
            copy.start()
    own_copies = []
    for m in range(1, 4):
        full = (exg_ref, upg_ref, dng_ref)[m - 1]
        copy = pltpu.make_async_copy(
            (ex_ref, up_ref, dn_ref)[m - 1],
            full.at[pl.ds(pl.multiple_of(w * chunk, chunk), chunk)], own_sem.at[m + 2],
        )
        copy.start()
        own_copies.append(copy)

    held = logit_mat.shape[1] // head
    wide = held * slices
    logit_mat[...] = jnp.zeros_like(logit_mat)
    for copy in small_copies[:2]:
        copy.wait()
    part_t = part_ref[...].astype(F32)
    sharp = sharp_ref[...]
    sharp_hi = sharp.astype(BF16).astype(F32)
    sharp_lo = sharp - sharp_hi
    for h in range(held):
        lanes = slice(h * head, (h + 1) * head)
        logit_mat[h * slices:(h + 1) * slices, lanes] = part_t
        logit_mat[wide + h:wide + h + 1, lanes] = sharp_hi
        logit_mat[wide + 8 + h:wide + 8 + h + 1, lanes] = sharp_lo
    num_buf[...] = jnp.zeros_like(num_buf)
    mass_buf[...] = jnp.zeros_like(mass_buf)
    x_copy.wait()

    def norm_step(t, carry):
        at = pl.ds(pl.multiple_of(t * norm_tile, norm_tile), norm_tile)
        rows_buf[at, :] = layer_norm(rows_buf[at, :].astype(F32)).astype(BF16)
        return carry

    norm_way = norm_tiles // 2
    lax.fori_loop(0, norm_way, norm_step, 0)

    def pass_on(m):
        copies = []
        for d in range(1, wid):
            crossing[m][d - 1].wait_recv()
            for e in range(1, chips):
                copy = forward(m, d, e)
                copy.start()
                copies.append(copy)
        return copies

    def trade(m):
        copies = []
        for d in range(1, wid):
            for e in range(1, chips):
                passed[m][(d - 1) * (chips - 1) + e - 1].wait_recv()
            copy = swap(m, d)
            copy.start()
            copies.append(copy)
        return copies

    width = ent_ref.shape[1]
    passed = [pass_on(0)]
    lax.fori_loop(norm_way, norm_tiles, norm_step, 0)
    traded = [trade(0)]
    passed += [pass_on(m) for m in range(1, 4)]
    for copy in traded[0]:
        copy.wait_recv()
    for d in range(wid):
        owner = lax.rem(w - d + wid, wid)
        entt_buf[pl.ds(pl.multiple_of(owner * width, width), width), :] = ent_buf[owner].T

    lhs = logit_mat[...].astype(BF16)
    groups = heads // held
    both = (((1,), (1,)), ((), ()))

    def slice_step(t, carry):
        at = pl.ds(pl.multiple_of(t * tile, tile), tile)
        feats = lax.dot_general(
            entt_buf[...], rows_buf[at, :], both, preferred_element_type=F32
        ).astype(BF16)
        for gi in range(groups):
            own = feats[gi * held * head:(gi + 1) * held * head]
            logits = jnp.dot(lhs, own, preferred_element_type=F32)
            raw = logits[wide:wide + 8] + logits[wide + 8:wide + 16]
            soft = jnp.maximum(raw, 0.0) + jnp.log1p(jnp.exp(-jnp.abs(raw)))
            inverse = 1.0 / (0.5 + soft)
            weights = []
            for h in range(held):
                score = logits[h * slices:(h + 1) * slices] * inverse[h:h + 1]
                power = jnp.exp(score - jnp.max(score, axis=0, keepdims=True))
                weights.append(power * (1.0 / jnp.sum(power, axis=0, keepdims=True)))
            block = jnp.concatenate(weights, axis=0).astype(BF16)
            num_buf[gi] += lax.dot_general(block, own, both, preferred_element_type=F32)
            rounded = block.astype(F32)
            mass = rounded[:, :128]
            for c in range(1, tile // 128):
                mass = mass + rounded[:, c * 128:(c + 1) * 128]
            mass_buf[gi * wide:(gi + 1) * wide] += mass
            w_ref[at, gi * wide:(gi + 1) * wide] = block.T
        return carry

    part_way = (tiles + 1) // 2
    lax.fori_loop(0, part_way, slice_step, 0)
    traded += [trade(m) for m in range(1, 4)]
    lax.fori_loop(part_way, tiles, slice_step, 0)

    lane = lax.broadcasted_iota(jnp.int32, (slices, 2 * head), 1)
    for h in range(heads):
        gi, k = h // held, h % held
        block = num_buf[gi, k * slices:(k + 1) * slices, (k // 2) * 2 * head:(k // 2 + 1) * 2 * head]
        if k % 2:
            block = pltpu.roll(block, head, 1)
        mass = jnp.sum(mass_buf[h * slices:(h + 1) * slices], axis=1, keepdims=True)
        piece_all[h * slices:(h + 1) * slices] = jnp.where(lane < head, block, mass)

    size = heads * slices // pts

    def piece(ref, owner):
        return ref.at[pl.ds(pl.multiple_of(owner * size, size), size)]

    scatter = []
    for d in range(1, pts):
        to = lax.rem(p + d, pts)
        scatter.append(pltpu.make_async_remote_copy(
            src_ref=piece(piece_all, to), dst_ref=piece_in.at[d - 1],
            send_sem=rs_send.at[d - 1], recv_sem=rs_recv.at[d - 1],
            device_id=(to, w), device_id_type=MESH,
        ))
    for copy in scatter:
        copy.start()
    total = piece_all[pl.ds(pl.multiple_of(p * size, size), size)]
    for d in range(1, pts):
        scatter[d - 1].wait_recv()
        total = total + piece_in[d - 1]
    piece_sum[...] = total
    ring = []
    for d in range(1, wid):
        ring.append(pltpu.make_async_remote_copy(
            src_ref=piece_sum, dst_ref=ring_in.at[d - 1],
            send_sem=z_send.at[d - 1], recv_sem=z_recv.at[d - 1],
            device_id=(p, lax.rem(w + d, wid)), device_id_type=MESH,
        ))
    for copy in ring:
        copy.start()
    for d in range(1, wid):
        ring[d - 1].wait_recv()
        total = total + ring_in[d - 1]
    fin_buf[pl.ds(pl.multiple_of(p * size, size), size)] = total
    spread = []
    for d in range(1, pts):
        spread.append(pltpu.make_async_remote_copy(
            src_ref=piece(fin_buf, p), dst_ref=piece(fin_buf, p),
            send_sem=ag_send.at[d - 1], recv_sem=ag_recv.at[d - 1],
            device_id=(lax.rem(p + d, pts), w), device_id_type=MESH,
        ))
    for copy in spread:
        copy.start()
    for copy in spread:
        copy.wait_recv()
    red_ref[...] = fin_buf[...]
    for m in range(1, 4):
        for copy in traded[m]:
            copy.wait_recv()
    for copy in own_copies:
        copy.wait()
    for copies in crossing + passed + traded + [scatter, ring, spread]:
        for copy in copies:
            copy.wait_send()


def rows_kernel(
    sizes, at_ref, red_ref, qkv_ref, w_ref, x_ref, exg_ref, upg_ref, dng_ref, out_ref, mix_buf
):
    head, slices, heads = sizes

    @pl.when(pl.program_id(0) == 0)
    def _():
        high = lax.Precision.HIGHEST
        count = heads * slices
        red = red_ref[...]
        tokens = red[:, :head] / (red[:, head:] + 1e-05)
        queries, keys_all, value_rows = (
            jnp.dot(tokens, qkv_ref[i], precision=high, preferred_element_type=F32)
            for i in range(3)
        )
        scores = lax.dot_general(
            queries, keys_all, (((1,), (1,)), ((), ())), precision=high,
            preferred_element_type=F32,
        ) * (1.0 / head ** 0.5)
        row = lax.broadcasted_iota(jnp.int32, (count, count), 0) // slices
        col = lax.broadcasted_iota(jnp.int32, (count, count), 1) // slices
        scores = jnp.where(row == col, scores, -jnp.inf)
        power = jnp.exp(scores - jnp.max(scores, axis=1, keepdims=True))
        attend = power / jnp.sum(power, axis=1, keepdims=True)
        out_tok = jnp.dot(attend, value_rows, precision=high, preferred_element_type=F32)
        spread = jnp.concatenate([out_tok] * heads, axis=1)
        row = lax.broadcasted_iota(jnp.int32, spread.shape, 0) // slices
        col = lax.broadcasted_iota(jnp.int32, spread.shape, 1) // head
        spread = jnp.where(row == col, spread, 0.0).astype(BF16)
        mix_buf[...] = jnp.dot(
            spread, exg_ref[...], preferred_element_type=F32
        ).astype(BF16)

    midway = x_ref[...].astype(F32) + jnp.dot(
        w_ref[...], mix_buf[...], preferred_element_type=F32
    )
    normed = layer_norm(midway).astype(BF16)
    hidden = jax.nn.gelu(jnp.dot(normed, upg_ref[...], preferred_element_type=F32)).astype(BF16)
    out_ref[...] = (
        midway + jnp.dot(hidden, dng_ref[...], preferred_element_type=F32)
    ).astype(BF16)


def local(x, entry, partition, sharpness, qkv, exit_m, widening, narrowing):
    pts, wid = lax.axis_size("pts"), lax.axis_size("wid")
    width = x.shape[1]
    head, slices = partition.shape
    heads = entry.shape[1] * wid // head
    rows = x.shape[0] // wid
    chunk = exit_m.shape[0]
    cells = heads * slices
    tile = pick_tile(rows, (1408, 256, 128))
    held = 256 // head
    size = cells // pts
    share = 2
    for choice in (8, 4):
        if pts % choice == 0 and chunk % (16 * choice) == 0:
            share = choice
            break
    sizes = (pts, wid, share, tile, head, slices, heads)
    vmem = pl.BlockSpec(memory_space=pltpu.VMEM)
    hbm = pl.BlockSpec(memory_space=pltpu.HBM)
    anywhere = pl.BlockSpec(memory_space=pl.ANY)
    dma = pltpu.SemaphoreType.DMA
    full = jax.ShapeDtypeStruct((chunk * wid, width), BF16)
    weights, reduced, exg, upg, dng = pl.pallas_call(
        functools.partial(gather_kernel, sizes),
        name="slices_and_gather",
        out_shape=(
            jax.ShapeDtypeStruct((rows, cells), BF16),
            jax.ShapeDtypeStruct((cells, 2 * head), F32),
            full, full, full,
        ),
        in_specs=[hbm] * 7,
        out_specs=(vmem, vmem, anywhere, anywhere, anywhere),
        scratch_shapes=[
            pltpu.VMEM((rows, width), BF16),
            pltpu.VMEM((wid,) + entry.shape, BF16),
            pltpu.VMEM((entry.shape[1] * wid, entry.shape[0]), BF16),
            pltpu.VMEM((held * slices + 16, held * head), F32),
            pltpu.VMEM((heads // held, held * slices, held * head), F32),
            pltpu.VMEM((cells, 128), F32),
            pltpu.VMEM((cells, 2 * head), F32),
            pltpu.VMEM((pts - 1, size, 2 * head), F32),
            pltpu.VMEM((size, 2 * head), F32),
            pltpu.VMEM((wid - 1, size, 2 * head), F32),
            pltpu.VMEM((cells, 2 * head), F32),
            pltpu.VMEM((slices, head), BF16),
            pltpu.VMEM((1, head), F32),
            dma, dma((6,)),
            dma((4, wid - 1)), dma((4, wid - 1)),
            dma((4, wid - 1, max(share // 2 - 1, 1))), dma((4, wid - 1, max(share // 2 - 1, 1))),
            dma((4, wid - 1)), dma((4, wid - 1)),
            dma((pts - 1,)), dma((pts - 1,)),
            dma((wid - 1,)), dma((wid - 1,)),
            dma((pts - 1,)), dma((pts - 1,)),
        ],
        compiler_params=pltpu.CompilerParams(
            collective_id=0, has_side_effects=True, vmem_limit_bytes=60 * 1024 * 1024
        ),
    )(x, entry, partition.T, sharpness.reshape(1, head), exit_m, widening, narrowing)

    step = pick_tile(rows, (1408, 704, 256, 128))
    steps = rows // step
    whole = lambda a: pl.BlockSpec(a.shape, lambda i, at: (0,) * a.ndim)
    at = lax.axis_index("wid").astype(jnp.int32).reshape(1)
    return pl.pallas_call(
        functools.partial(rows_kernel, (head, slices, heads)),
        name="mix_and_feed",
        out_shape=jax.ShapeDtypeStruct((rows, width), BF16),
        grid_spec=pltpu.PrefetchScalarGridSpec(
            num_scalar_prefetch=1,
            grid=(steps,),
            in_specs=[
                whole(reduced),
                whole(qkv),
                pl.BlockSpec((step, cells), lambda i, at: (i, 0)),
                pl.BlockSpec((step, width), lambda i, at: (at[0] * steps + i, 0)),
                whole(exg), whole(upg), whole(dng),
            ],
            out_specs=pl.BlockSpec((step, width), lambda i, at: (i, 0)),
            scratch_shapes=[pltpu.VMEM((cells, width), BF16)],
        ),
        compiler_params=pltpu.CompilerParams(
            dimension_semantics=("arbitrary",), vmem_limit_bytes=61 * 1024 * 1024
        ),
    )(at, reduced, qkv, weights, x, exg, upg, dng)


def solution(mesh):
    placed = (
        P("pts", None),
        P(None, "wid"),
        P(),
        P(),
        P(),
        P("wid", None),
        P("wid", None),
        P("wid", None),
    )
    return jax.shard_map(
        local, mesh=mesh, in_specs=placed, out_specs=P(("pts", "wid"), None), check_vma=False
    )
```
